32 devices in a mesh: section: 4 (over y, x), tensor: 2 (over core), dp: 4 (over z).
Axes of the slice: x: 2, y: 2, z: 4, core: 2. Of those that a mesh axis runs over, the one named last changes fastest.
Arguments:
- hidden_in: bfloat16 [128, 4096], P('dp', 'tensor'), may hold values from -6 to 6
- norm_gain: float32 [4, 4096], P('section'), may hold values from 0.25 to 1.75
- gate_weight: bfloat16 [4, 4096, 8192], P('section', 'dp', 'tensor'), may hold values from -0.09375 to 0.09375
- up_weight: bfloat16 [4, 4096, 8192], P('section', 'dp', 'tensor'), may hold values from -0.09375 to 0.09375
- down_weight: bfloat16 [4, 4096, 8192], P('section', 'dp', 'tensor'), may hold values from -0.0625 to 0.0625
- lengths: int32 [16], P('dp'), may hold values from 3 to 8
Outputs:
- rdm: float32 [4, 16, 16], P('section', 'dp')
The draws below stay inside these ranges and needn't reach their ends.
Inputs may be any that keep to these rules, and one draw needn't show every extreme that they name: `lengths`: the number of leading valid token rows of each sentence.
All inputs are finite; a program needn't handle non-finite values.
Results may differ from the reference program's by a relative error of at most 0.0012.
Values may be sent and summed in bfloat16 or wider, within the bound.
A program may use at most 192 MiB of HBM per device.

```python
import jax
import jax.numpy as jnp
from jax import lax

D = 4096
FF = 8192
LEN = 8
SENT = 16
TOKENS = 128
SECTIONS = 4
N_SECTION = 4


def plant(drawn, own_key, smallest, top_value):
    longest = drawn.shape.index(max(drawn.shape))
    spots = []
    for shift in (0, 1):
        where = [jax.random.randint(jax.random.fold_in(own_key, axis), (), 0, length) for axis, length in enumerate(drawn.shape)]
        where[longest] = (where[longest] + shift) % drawn.shape[longest]
        spots.append(tuple(where))
    return drawn.at[spots[0]].set(smallest).at[spots[1]].set(top_value)


def block_scale(own_key, shape, pieces, least, largest):
    loudness, own = 1.0, jax.random.fold_in(own_key, 6)
    for axis_at, parts in pieces:
        draws = jnp.exp(jax.random.uniform(jax.random.fold_in(own, axis_at), (parts,), jnp.float32, least / len(pieces), largest / len(pieces)))
        loudness = loudness * jnp.repeat(draws, shape[axis_at] // parts).reshape([-1 if axis == axis_at else 1 for axis in range(len(shape))])
    return loudness


def gaussian(stream_key, dims, deviation, most, split=(), kind=jnp.bfloat16):
    values = deviation * jax.random.normal(stream_key, dims, jnp.float32)
    if split:
        values = values * block_scale(stream_key, dims, split, -0.22, 0.18)
    return jnp.clip(values, -most, most).astype(kind)


def setup_inputs(seed: int = 0) -> dict:
    keys = jax.random.split(jax.random.key(seed), 7)
    return {
        "hidden_in": gaussian(keys[0], (TOKENS, D), 1.0, 6.0, ((0, 4), (1, 2))),
        "norm_gain": jnp.clip(1.0 + 0.15 * jax.random.normal(keys[1], (SECTIONS, D), jnp.float32), 0.25, 1.75),
        "gate_weight": gaussian(keys[2], (SECTIONS, D, FF), D ** -0.5, 0.09375, ((0, 4), (1, 4), (2, 2))),
        "up_weight": gaussian(keys[3], (SECTIONS, D, FF), D ** -0.5, 0.09375, ((0, 4), (1, 4), (2, 2))),
        "down_weight": gaussian(keys[4], (SECTIONS, D, FF), FF ** -0.5, 0.0625, ((0, 4), (1, 4), (2, 2))),
        "lengths": plant(jax.random.randint(keys[5], (SENT,), 3, LEN + 1), jax.random.fold_in(keys[5], 1), 3, LEN).astype(jnp.int32),
    }


RMS_EPS = 1e-05
UNIT_FLOOR = 0.1
CONTRACT_LAST = (((1,), (1,)), ((), ()))

def reference(hidden_in, norm_gain, gate_weight, up_weight, down_weight, lengths):
    current = hidden_in
    positions = jnp.arange(LEN, dtype=jnp.int32)
    weights = (positions[None, :] < lengths[:, None]).astype(jnp.float32)
    counts = lengths.astype(jnp.float32)
    results = []
    for layer in range(N_SECTION):
        wide_state = current.astype(jnp.float32)
        inv_rms = lax.rsqrt(lax.optimization_barrier(jnp.mean(wide_state * wide_state, axis=1, keepdims=True)) + RMS_EPS)
        normed = (wide_state * inv_rms * norm_gain[layer][None, :]).astype(jnp.bfloat16)
        gate_sum = jnp.dot(normed, gate_weight[layer], preferred_element_type=jnp.float32)
        up_sum = jnp.dot(normed, up_weight[layer], preferred_element_type=jnp.float32)
        hidden = (jax.nn.silu(gate_sum) * up_sum).astype(jnp.bfloat16)
        summed = lax.dot_general(hidden, down_weight[layer], CONTRACT_LAST, preferred_element_type=jnp.float32)
        current = (wide_state + summed).astype(jnp.bfloat16)
        shaped = current.astype(jnp.float32).reshape(SENT, LEN, D)
        pooled = lax.optimization_barrier(jnp.sum(shaped * weights[:, :, None], axis=1)) / counts[:, None]
        centered = pooled - lax.optimization_barrier(jnp.mean(pooled, axis=1, keepdims=True))
        unit_rows = (centered * lax.rsqrt(lax.optimization_barrier(jnp.mean(centered * centered, axis=1, keepdims=True)) + UNIT_FLOOR)).astype(jnp.bfloat16)
        products = lax.dot_general(unit_rows, unit_rows, CONTRACT_LAST, preferred_element_type=jnp.float32)
        results.append(1.0 - products / D)
    return jnp.stack(results)
```

```python
import jax
import jax.numpy as jnp
from jax import lax
from jax.sharding import PartitionSpec as P

RMS_EPS = 1e-05
UNIT_FLOOR = 0.1
CONTRACT_LAST = (((1,), (1,)), ((), ()))


def per_device(hidden_in, norm_gain, gate_weight, up_weight, down_weight, lengths):
    section = lax.axis_index("section")
    dp = lax.axis_index("dp")
    sections = lax.axis_size("section")
    dps = lax.axis_size("dp")
    gate, up, down = gate_weight[0], up_weight[0], down_weight[0]
    width = gate.shape[0]
    d_model = width * dps
    gain = lax.dynamic_slice_in_dim(norm_gain[0], dp * width, width, 0)
    source = lax.all_gather(hidden_in, "tensor", axis=1, tiled=True)
    state = lax.all_to_all(source, "dp", split_axis=1, concat_axis=0, tiled=True)
    lens = lax.all_gather(lengths, "dp", axis=0, tiled=True)
    final = state
    pairs = [(i, i + 1) for i in range(sections - 1)]
    for tick in range(sections):
        wide = state.astype(jnp.float32)
        total = lax.psum(jnp.sum(wide * wide, axis=1, keepdims=True), "dp")
        normed = (wide * lax.rsqrt(total / d_model + RMS_EPS) * gain[None, :]).astype(jnp.bfloat16)
        g = jnp.dot(normed, gate, preferred_element_type=jnp.float32).astype(jnp.bfloat16)
        u = jnp.dot(normed, up, preferred_element_type=jnp.float32).astype(jnp.bfloat16)
        both = lax.psum_scatter(jnp.concatenate([g, u], axis=1), "dp", scatter_dimension=0, tiled=True)
        both = both.astype(jnp.float32)
        cols = gate.shape[1]
        hidden = (jax.nn.silu(both[:, :cols]) * both[:, cols:]).astype(jnp.bfloat16)
        hidden = lax.all_gather(hidden, "dp", axis=0, tiled=True)
        part = lax.dot_general(hidden, down, CONTRACT_LAST, preferred_element_type=jnp.float32)
        summed = lax.psum(part.astype(jnp.bfloat16), "tensor").astype(jnp.float32)
        out = (wide + summed).astype(jnp.bfloat16)
        final = jnp.where(section == tick, out, final)
        if tick < sections - 1:
            state = lax.ppermute(out, "section", pairs)
    sents = lens.shape[0]
    shaped = final.astype(jnp.float32).reshape(sents, -1, width)
    positions = jnp.arange(shaped.shape[1], dtype=jnp.int32)
    weights = (positions[None, :] < lens[:, None]).astype(jnp.float32)
    pooled = jnp.sum(shaped * weights[:, :, None], axis=1) / lens.astype(jnp.float32)[:, None]
    mean = lax.psum(jnp.sum(pooled, axis=1, keepdims=True), "dp") / d_model
    centered = pooled - mean
    var = lax.psum(jnp.sum(centered * centered, axis=1, keepdims=True), "dp") / d_model
    unit = (centered * lax.rsqrt(var + UNIT_FLOOR)).astype(jnp.bfloat16)
    products = lax.dot_general(unit, unit, CONTRACT_LAST, preferred_element_type=jnp.float32)
    products = lax.psum_scatter(products, "dp", scatter_dimension=0, tiled=True)
    return (1.0 - products / d_model)[None]


def solution(mesh):
    placed = (
        P("dp", "tensor"),
        P("section", None),
        P("section", "dp", "tensor"),
        P("section", "dp", "tensor"),
        P("section", "dp", "tensor"),
        P("dp"),
    )
    return jax.shard_map(
        per_device, mesh=mesh, in_specs=placed, out_specs=P("section", "dp", None), check_vma=False
    )
```

```python
import functools

import jax
import jax.numpy as jnp
from jax import lax
from jax.experimental import pallas as pl
from jax.experimental.pallas import tpu as pltpu
from jax.sharding import PartitionSpec as P

RMS_EPS = 1e-05
UNIT_FLOOR = 0.1
CONTRACT_LAST = (((1,), (1,)), ((), ()))
MESH = pl.DeviceIdType.MESH
LANES = 128
F32 = jnp.float32
BF16 = jnp.bfloat16


def kernel(dps, tensors, sections, hidden_ref, gain_ref, mask_ref, lens_ref, gate_hbm, up_hbm, down_hbm,
           out_ref, gate_v, up_v, down_v, x_in, rs_out, rs_in, own_gu, own_ss, hid, tx, outs, stat, gram,
           w_sem, d_send, x_send, x_recv, rs_send, rs_recv, h_send, h_recv, t_send, t_recv,
           s_send, s_recv, g_send, g_recv):
    section = lax.axis_index("section")
    tensor = lax.axis_index("tensor")
    dp = lax.axis_index("dp")
    micros = dps
    width = gate_v.shape[0]
    cols = gate_v.shape[1]
    fc = cols // dps
    rows = x_in.shape[1]
    d_model = width * dps
    nj = hidden_ref.shape[1] // width

    def chunk(c):
        return pl.ds(pl.multiple_of(c * fc, fc), fc)

    def wcopy(which, c):
        src, dst = ((gate_hbm, gate_v), (up_hbm, up_v), (down_hbm, down_v))[which]
        return pltpu.make_async_copy(src.at[0, :, chunk(c)], dst.at[:, chunk(c)], w_sem.at[which, c])

    order = [lax.rem(dp + k, dps) for k in range(1, dps + 1)]
    for c in order:
        wcopy(0, c).start()
        wcopy(1, c).start()
    for c in order:
        wcopy(2, c).start()

    barrier = pltpu.get_barrier_semaphore()
    for kt in range(tensors):
        for kd in range(dps):
            if kt or kd:
                pl.semaphore_signal(
                    barrier, inc=1,
                    device_id={"tensor": lax.rem(tensor + kt, tensors), "dp": lax.rem(dp + kd, dps)},
                    device_id_type=MESH)

    @pl.when(section > 0)
    def _():
        pl.semaphore_signal(barrier, inc=1, device_id={"section": section - 1}, device_id_type=MESH)

    @pl.when(section < sections - 1)
    def _():
        pl.semaphore_signal(barrier, inc=1, device_id={"section": section + 1}, device_id_type=MESH)

    pl.semaphore_wait(
        barrier,
        tensors * dps + 1 - jnp.where(section == 0, 1, 0) - jnp.where(section == sections - 1, 1, 0))

    def spread(j, k):
        return pltpu.make_async_remote_copy(
            src_ref=hidden_ref.at[:, pl.ds(j * width, width)], dst_ref=x_in.at[dp],
            send_sem=d_send.at[j, k], recv_sem=x_recv.at[dp],
            device_id={"tensor": lax.rem(tensor + k, tensors), "dp": tensor * nj + j}, device_id_type=MESH)

    @pl.when(section == 0)
    def _():
        for j in range(nj):
            for k in range(tensors):
                if k:
                    spread(j, k).start()
                else:
                    @pl.when(tensor * nj + j != dp)
                    def _():
                        spread(j, k).start()

                    @pl.when(tensor * nj + j == dp)
                    def _():
                        x_in[dp] = hidden_ref[:, j * width:(j + 1) * width]

    def rs_copy(m, c):
        return pltpu.make_async_remote_copy(
            src_ref=rs_out.at[m, c], dst_ref=rs_in.at[m, dp],
            send_sem=rs_send.at[m, c], recv_sem=rs_recv.at[m, dp],
            device_id={"dp": c}, device_id_type=MESH)

    def rs_wait(m, c):
        return pltpu.make_async_remote_copy(
            src_ref=rs_out.at[m, c], dst_ref=rs_in.at[m, c],
            send_sem=rs_send.at[m, c], recv_sem=rs_recv.at[m, c],
            device_id={"dp": c}, device_id_type=MESH)

    def h_copy(m, c, peer):
        return pltpu.make_async_remote_copy(
            src_ref=hid.at[m, c], dst_ref=hid.at[m, c],
            send_sem=h_send.at[m, peer], recv_sem=h_recv.at[m, c],
            device_id={"dp": peer}, device_id_type=MESH)

    def t_copy(m, c, peer):
        return pltpu.make_async_remote_copy(
            src_ref=tx.at[m, c], dst_ref=tx.at[m, c],
            send_sem=t_send.at[m, peer], recv_sem=t_recv.at[m, c],
            device_id={"tensor": peer}, device_id_type=MESH)

    def x_copy(m, to):
        return pltpu.make_async_remote_copy(
            src_ref=outs.at[m], dst_ref=x_in.at[m],
            send_sem=x_send.at[m], recv_sem=x_recv.at[m],
            device_id={"section": to}, device_id_type=MESH)

    lane = lax.broadcasted_iota(jnp.int32, (rows, LANES), 1)

    def gate_up(m):
        local = jnp.logical_and(section == 0, jnp.logical_and(m == dp, lax.div(dp, nj) == tensor))

        @pl.when(jnp.logical_not(local))
        def _():
            x_copy(m, section).wait_recv()

        x = x_in[m].astype(F32)
        ss = jnp.sum(x * x, axis=1, keepdims=True)
        high = ss.astype(BF16)
        low = (ss - high.astype(F32)).astype(BF16)
        packed = jnp.where(lane < LANES // 2, high.astype(F32), low.astype(F32)).astype(BF16)
        own_ss[m] = jnp.broadcast_to(ss, (rows, LANES))
        scaled = (x * gain_ref[...]).astype(BF16)
        for k in range(1, dps + 1):
            c = lax.rem(dp + k, dps)

            @pl.when(m == 0)
            def _():
                wcopy(0, c).wait()
                wcopy(1, c).wait()

            g = jnp.dot(scaled, gate_v[:, chunk(c)], preferred_element_type=F32)
            u = jnp.dot(scaled, up_v[:, chunk(c)], preferred_element_type=F32)
            if k < dps:
                rs_out[m, c, :, 0:fc] = g.astype(BF16)
                rs_out[m, c, :, fc:2 * fc] = u.astype(BF16)
                rs_out[m, c, :, 2 * fc:] = packed
                rs_copy(m, c).start()
            else:
                own_gu[m, :, 0:fc] = g
                own_gu[m, :, fc:] = u

    def activate(m):
        for k in range(1, dps):
            rs_wait(m, lax.rem(dp + k, dps)).wait_recv()
        g = own_gu[m, :, 0:fc]
        u = own_gu[m, :, fc:]
        ss = own_ss[m][:, 0:1]
        for k in range(1, dps):
            c = lax.rem(dp + k, dps)
            g = g + rs_in[m, c, :, 0:fc].astype(F32)
            u = u + rs_in[m, c, :, fc:2 * fc].astype(F32)
            ss = ss + jnp.sum(rs_in[m, c, :, 2 * fc:].astype(F32), axis=1, keepdims=True) * (2.0 / LANES)
        inv = lax.rsqrt(ss * (1.0 / d_model) + RMS_EPS)
        g = g * inv
        u = u * inv
        hid[m, dp] = (g / (1.0 + jnp.exp(-g)) * u).astype(BF16)
        for k in range(1, dps):
            h_copy(m, dp, lax.rem(dp + k, dps)).start()

    def finish(m):
        acc = jnp.zeros((rows, width), F32)
        for k in range(dps):
            c = lax.rem(dp + k, dps)
            if k:
                h_copy(m, c, c).wait_recv()

            @pl.when(m == 0)
            def _():
                wcopy(2, c).wait()

            acc = acc + lax.dot_general(hid[m, c], down_v[:, chunk(c)], CONTRACT_LAST,
                                        preferred_element_type=F32)
        tx[m, tensor] = acc.astype(BF16)
        for k in range(1, tensors):
            t_copy(m, tensor, lax.rem(tensor + k, tensors)).start()
        for k in range(1, tensors):
            other = lax.rem(tensor + k, tensors)
            t_copy(m, other, other).wait_recv()
        total = tx[m, 0].astype(F32)
        for t in range(1, tensors):
            total = total + tx[m, t].astype(F32)
        outs[m] = (x_in[m].astype(F32) + total).astype(BF16)

        @pl.when(section < sections - 1)
        def _():
            x_copy(m, section + 1).start()

    def step(m, carry):
        gate_up(m)
        activate(m)
        finish(m)
        return carry

    lax.fori_loop(0, micros, step, 0)

    sents = mask_ref.shape[0]
    pooled = jnp.zeros((sents, width), F32)
    for m in range(micros):
        pooled = pooled + jnp.dot(mask_ref[:, m * rows:(m + 1) * rows], outs[m], preferred_element_type=F32)
    pooled = pooled / lens_ref[:, 0:1]

    def s_copy(buf, send, recv, c, peer):
        return pltpu.make_async_remote_copy(
            src_ref=buf.at[c], dst_ref=buf.at[c], send_sem=send.at[peer], recv_sem=recv.at[c],
            device_id={"dp": peer}, device_id_type=MESH)

    def share(buf, send, recv):
        for k in range(1, dps):
            s_copy(buf, send, recv, dp, lax.rem(dp + k, dps)).start()
        for k in range(1, dps):
            c = lax.rem(dp + k, dps)
            s_copy(buf, send, recv, c, c).wait_recv()

    stat[dp] = jnp.broadcast_to(jnp.sum(pooled, axis=1, keepdims=True), (sents, LANES))
    share(stat, s_send, s_recv)
    total = stat[0]
    for c in range(1, dps):
        total = total + stat[c]
    centered = pooled - total[:, 0:1] * (1.0 / d_model)
    narrow = centered.astype(BF16)
    sq = jnp.sum(centered * centered, axis=1, keepdims=True)
    gram[dp, 0] = jnp.zeros((sents, LANES), F32)
    gram[dp, 0, :, 0:sents] = lax.dot_general(narrow, narrow, CONTRACT_LAST, preferred_element_type=F32)
    gram[dp, 1] = jnp.broadcast_to(sq, (sents, LANES))
    share(gram, g_send, g_recv)
    products = gram[0, 0]
    sq = gram[0, 1]
    for c in range(1, dps):
        products = products + gram[c, 0]
        sq = sq + gram[c, 1]
    scale = lax.rsqrt(sq * (1.0 / d_model) + UNIT_FLOOR)
    r_i = lax.broadcasted_iota(jnp.int32, (sents, LANES), 0)
    c_i = lax.broadcasted_iota(jnp.int32, (sents, LANES), 1)
    across = jnp.sum(jnp.where(r_i == c_i, scale, 0.0), axis=0, keepdims=True)
    out_ref[...] = 1.0 - products * scale * across * (1.0 / d_model)

    @pl.when(section == 0)
    def _():
        for j in range(nj):
            for k in range(tensors):
                if k:
                    spread(j, k).wait_send()
                else:
                    @pl.when(tensor * nj + j != dp)
                    def _():
                        spread(j, k).wait_send()

    def drain(m, carry):
        for k in range(1, dps):
            c = lax.rem(dp + k, dps)
            rs_copy(m, c).wait_send()
            h_copy(m, dp, c).wait_send()
        for k in range(1, tensors):
            t_copy(m, tensor, lax.rem(tensor + k, tensors)).wait_send()

        @pl.when(section < sections - 1)
        def _():
            x_copy(m, section + 1).wait_send()
        return carry

    lax.fori_loop(0, micros, drain, 0)
    for k in range(1, dps):
        c = lax.rem(dp + k, dps)
        s_copy(stat, s_send, s_recv, dp, c).wait_send()
        s_copy(gram, g_send, g_recv, dp, c).wait_send()


def per_device(hidden_in, norm_gain, gate_weight, up_weight, down_weight, lengths):
    dp = lax.axis_index("dp")
    sections = lax.axis_size("section")
    tensors = lax.axis_size("tensor")
    dps = lax.axis_size("dp")
    _, width, cols = gate_weight.shape
    rows = hidden_in.shape[0]
    fc = cols // dps
    nj = hidden_in.shape[1] // width
    gain = lax.dynamic_slice_in_dim(norm_gain, dp * width, width, 1)
    lens = lax.all_gather(lengths, "dp", axis=0, tiled=True)
    sents = lens.shape[0]
    per = rows * dps // sents
    token = jnp.arange(rows * dps, dtype=jnp.int32)[None, :] - per * jnp.arange(sents, dtype=jnp.int32)[:, None]
    mask = jnp.logical_and(token >= 0, token < lens[:, None]).astype(BF16)
    lens_wide = jnp.broadcast_to(lens.astype(F32)[:, None], (sents, LANES))
    vm = pl.BlockSpec(memory_space=pltpu.VMEM)
    hbm = pl.BlockSpec(memory_space=pl.ANY)
    dma = pltpu.SemaphoreType.DMA
    result = pl.pallas_call(
        functools.partial(kernel, dps, tensors, sections),
        out_shape=jax.ShapeDtypeStruct((sents, LANES), F32),
        in_specs=[vm] * 4 + [hbm] * 3,
        out_specs=vm,
        scratch_shapes=[
            pltpu.VMEM((width, cols), BF16),
            pltpu.VMEM((width, cols), BF16),
            pltpu.VMEM((width, cols), BF16),
            pltpu.VMEM((dps, rows, width), BF16),
            pltpu.VMEM((dps, dps, rows, 2 * fc + LANES), BF16),
            pltpu.VMEM((dps, dps, rows, 2 * fc + LANES), BF16),
            pltpu.VMEM((dps, rows, 2 * fc), F32),
            pltpu.VMEM((dps, rows, LANES), F32),
            pltpu.VMEM((dps, dps, rows, fc), BF16),
            pltpu.VMEM((dps, tensors, rows, width), BF16),
            pltpu.VMEM((dps, rows, width), BF16),
            pltpu.VMEM((dps, sents, LANES), F32),
            pltpu.VMEM((dps, 2, sents, LANES), F32),
            dma((3, dps)),
            dma((nj, tensors)),
            dma((dps,)),
            dma((dps,)),
            dma((dps, dps)),
            dma((dps, dps)),
            dma((dps, dps)),
            dma((dps, dps)),
            dma((dps, tensors)),
            dma((dps, tensors)),
            dma((dps,)),
            dma((dps,)),
            dma((dps,)),
            dma((dps,)),
        ],
        compiler_params=pltpu.CompilerParams(
            collective_id=0, has_side_effects=True, vmem_limit_bytes=60 * 1024 * 1024),
    )(hidden_in, gain, mask, lens_wide, gate_weight, up_weight, down_weight)
    each = sents // dps
    return lax.dynamic_slice_in_dim(result, dp * each, each, 0)[None, :, :sents]


def solution(mesh):
    placed = (
        P("dp", "tensor"),
        P("section", None),
        P("section", "dp", "tensor"),
        P("section", "dp", "tensor"),
        P("section", "dp", "tensor"),
        P("dp"),
    )
    return jax.shard_map(
        per_device, mesh=mesh, in_specs=placed, out_specs=P("section", "dp", None), check_vma=False
    )
```

```python
import functools

import jax
import jax.numpy as jnp
from jax import lax
from jax.experimental import pallas as pl
from jax.experimental.pallas import tpu as pltpu
from jax.sharding import PartitionSpec as P

RMS_EPS = 1e-05
UNIT_FLOOR = 0.1
CONTRACT_LAST = (((1,), (1,)), ((), ()))
MESH = pl.DeviceIdType.MESH
LANES = 128
F32 = jnp.float32
BF16 = jnp.bfloat16


SPLIT = 2


def kernel(dps, tensors, sections, hidden_ref, gain_ref, lens_ref, gate_hbm, up_hbm, down_hbm,
           out_ref, gate_v, up_v, down_v, x_in, rs_out, rs_in, own_gu, own_ss, hid, tx, outs, stat, gram, lbuf, lens_full,
           w_sem, d_send, x_send, x_recv, rs_send, rs_recv, h_send, h_recv, t_send, t_recv,
           s_send, s_recv, g_send, g_recv, l_send, l_recv):
    section = lax.axis_index("section")
    tensor = lax.axis_index("tensor")
    dp = lax.axis_index("dp")
    micros = dps * SPLIT
    width = gate_v.shape[0]
    cols = gate_v.shape[1]
    fc = cols // dps
    rows = x_in.shape[1]
    d_model = width * dps
    nj = hidden_ref.shape[1] // width

    def chunk(c):
        return pl.ds(pl.multiple_of(c * fc, fc), fc)

    def wcopy(which, c):
        src, dst = ((gate_hbm, gate_v), (up_hbm, up_v), (down_hbm, down_v))[which]
        return pltpu.make_async_copy(src.at[0, :, chunk(c)], dst.at[:, chunk(c)], w_sem.at[which, c])

    if dps == 4:
        mirror = dps - 1 - dp
        peers = [mirror, lax.rem(dp + 2, dps), lax.rem(mirror + 2, dps)]
    else:
        peers = [lax.rem(dp + k, dps) for k in range(1, dps)]
    order = peers + [dp]
    for c in order:
        wcopy(0, c).start()
        wcopy(1, c).start()
    for c in order:
        wcopy(2, c).start()

    barrier = pltpu.get_barrier_semaphore()
    for kt in range(tensors):
        for kd in range(dps):
            if kt or kd:
                pl.semaphore_signal(
                    barrier, inc=1,
                    device_id={"tensor": lax.rem(tensor + kt, tensors), "dp": lax.rem(dp + kd, dps)},
                    device_id_type=MESH)

    @pl.when(section > 0)
    def _():
        pl.semaphore_signal(barrier, inc=1, device_id={"section": section - 1}, device_id_type=MESH)

    @pl.when(section < sections - 1)
    def _():
        pl.semaphore_signal(barrier, inc=1, device_id={"section": section + 1}, device_id_type=MESH)

    pl.semaphore_wait(
        barrier,
        tensors * dps + 1 - jnp.where(section == 0, 1, 0) - jnp.where(section == sections - 1, 1, 0))

    each = lens_ref.shape[0]
    sents = each * dps
    slot = lax.broadcasted_iota(jnp.int32, lbuf.shape[1:], 0)
    own_lens = jnp.ones(lbuf.shape[1:], F32)
    for n in range(each):
        own_lens = jnp.where(slot == n, lens_ref[n].astype(F32), own_lens)
    lbuf[dp] = own_lens

    def s_copy(buf, send, recv, c, peer):
        return pltpu.make_async_remote_copy(
            src_ref=buf.at[c], dst_ref=buf.at[c], send_sem=send.at[peer], recv_sem=recv.at[c],
            device_id={"dp": peer}, device_id_type=MESH)

    def spread(h, j, k):
        return pltpu.make_async_remote_copy(
            src_ref=hidden_ref.at[pl.ds(h * rows, rows), pl.ds(j * width, width)],
            dst_ref=x_in.at[dp * SPLIT + h],
            send_sem=d_send.at[h, j * tensors + k], recv_sem=x_recv.at[dp * SPLIT + h],
            device_id={"tensor": lax.rem(tensor + k, tensors), "dp": tensor * nj + j}, device_id_type=MESH)

    @pl.when(section == 0)
    def _():
        for h in range(SPLIT):
            for j in range(nj):
                for k in range(tensors):
                    if k:
                        spread(h, j, k).start()
                    else:
                        @pl.when(tensor * nj + j != dp)
                        def _():
                            spread(h, j, k).start()

                        @pl.when(tensor * nj + j == dp)
                        def _():
                            x_in[dp * SPLIT + h] = hidden_ref[h * rows:(h + 1) * rows, j * width:(j + 1) * width]

    for c in peers:
        s_copy(lbuf, l_send, l_recv, dp, c).start()

    def rs_copy(m, c):
        return pltpu.make_async_remote_copy(
            src_ref=rs_out.at[m, c], dst_ref=rs_in.at[m, dp],
            send_sem=rs_send.at[m, c], recv_sem=rs_recv.at[m, dp],
            device_id={"dp": c}, device_id_type=MESH)

    def rs_wait(m, c):
        return pltpu.make_async_remote_copy(
            src_ref=rs_out.at[m, c], dst_ref=rs_in.at[m, c],
            send_sem=rs_send.at[m, c], recv_sem=rs_recv.at[m, c],
            device_id={"dp": c}, device_id_type=MESH)

    def h_copy(m, c, peer):
        return pltpu.make_async_remote_copy(
            src_ref=hid.at[m, c], dst_ref=hid.at[m, c],
            send_sem=h_send.at[m, peer], recv_sem=h_recv.at[m, c],
            device_id={"dp": peer}, device_id_type=MESH)

    def t_copy(m, c, peer):
        return pltpu.make_async_remote_copy(
            src_ref=tx.at[m, c], dst_ref=tx.at[m, c],
            send_sem=t_send.at[m, peer], recv_sem=t_recv.at[m, c],
            device_id={"tensor": peer}, device_id_type=MESH)

    def x_copy(m, to):
        return pltpu.make_async_remote_copy(
            src_ref=outs.at[m], dst_ref=x_in.at[m],
            send_sem=x_send.at[m], recv_sem=x_recv.at[m],
            device_id={"section": to}, device_id_type=MESH)

    lane = lax.broadcasted_iota(jnp.int32, (rows, LANES), 1)

    def gate_up(m):
        local = jnp.logical_and(section == 0, jnp.logical_and(m // SPLIT == dp, dp // nj == tensor))

        @pl.when(jnp.logical_not(local))
        def _():
            x_copy(m, section).wait_recv()

        x = x_in[m].astype(F32)
        ss = jnp.sum(x * x, axis=1, keepdims=True)
        high = ss.astype(BF16)
        low = (ss - high.astype(F32)).astype(BF16)
        packed = jnp.where(lane < LANES // 2, high.astype(F32), low.astype(F32)).astype(BF16)
        own_ss[m] = jnp.broadcast_to(ss, (rows, LANES))
        scaled = (x * gain_ref[:, pl.ds(pl.multiple_of(dp * width, width), width)]).astype(BF16)
        for k, c in enumerate(order):
            @pl.when(m == 0)
            def _():
                wcopy(0, c).wait()
                wcopy(1, c).wait()

            g = jnp.dot(scaled, gate_v[:, chunk(c)], preferred_element_type=F32)
            u = jnp.dot(scaled, up_v[:, chunk(c)], preferred_element_type=F32)
            if k < dps - 1:
                rs_out[m, c, :, 0:fc] = g.astype(BF16)
                rs_out[m, c, :, fc:2 * fc] = u.astype(BF16)
                rs_out[m, c, :, 2 * fc:] = packed
                rs_copy(m, c).start()
            else:
                own_gu[m, :, 0:fc] = g
                own_gu[m, :, fc:] = u

    def activate(m):
        for c in peers:
            rs_wait(m, c).wait_recv()
        g = own_gu[m, :, 0:fc]
        u = own_gu[m, :, fc:]
        ss = own_ss[m][:, 0:1]
        for c in peers:
            g = g + rs_in[m, c, :, 0:fc].astype(F32)
            u = u + rs_in[m, c, :, fc:2 * fc].astype(F32)
            ss = ss + jnp.sum(rs_in[m, c, :, 2 * fc:].astype(F32), axis=1, keepdims=True) * (2.0 / LANES)
        inv = lax.rsqrt(ss * (1.0 / d_model) + RMS_EPS)
        g = g * inv
        u = u * inv
        hid[m, dp] = (g / (1.0 + jnp.exp(-g)) * u).astype(BF16)
        for c in peers:
            h_copy(m, dp, c).start()

    def finish(m):
        acc = jnp.zeros((rows, width), F32)
        for k, c in enumerate([dp] + peers[::2] + peers[1::2]):
            if k:
                h_copy(m, c, c).wait_recv()

            @pl.when(m == 0)
            def _():
                wcopy(2, c).wait()

            acc = acc + lax.dot_general(hid[m, c], down_v[:, chunk(c)], CONTRACT_LAST,
                                        preferred_element_type=F32)
        tx[m, tensor] = acc.astype(BF16)
        for k in range(1, tensors):
            t_copy(m, tensor, lax.rem(tensor + k, tensors)).start()
        for k in range(1, tensors):
            other = lax.rem(tensor + k, tensors)
            t_copy(m, other, other).wait_recv()
        total = tx[m, 0].astype(F32)
        for t in range(1, tensors):
            total = total + tx[m, t].astype(F32)
        outs[m] = (x_in[m].astype(F32) + total).astype(BF16)

        @pl.when(section < sections - 1)
        def _():
            x_copy(m, section + 1).start()

    def step(i, carry):
        @pl.when(i < micros)
        def _():
            gate_up(i)

        @pl.when(i > 0)
        def _():
            finish(i - 1)

        @pl.when(i < micros)
        def _():
            activate(i)
        return carry

    lax.fori_loop(0, micros + 1, step, 0)

    for c in peers:
        s_copy(lbuf, l_send, l_recv, c, c).wait_recv()
    for c in range(dps):
        lens_full[c * each:(c + 1) * each] = lbuf[c, 0:each]
    tokens = micros * rows
    per = tokens // sents
    place = lax.broadcasted_iota(jnp.int32, (sents, tokens), 1) - per * lax.broadcasted_iota(
        jnp.int32, (sents, tokens), 0)
    lens = lens_full[:, 0:1]
    valid = jnp.logical_and(place >= 0, place.astype(F32) < lens)
    mask = jnp.where(valid, 1.0, 0.0).astype(BF16)
    pooled = jnp.dot(mask, outs[...].reshape(tokens, width), preferred_element_type=F32) / lens

    def share(buf, send, recv):
        for c in peers:
            s_copy(buf, send, recv, dp, c).start()
        for c in peers:
            s_copy(buf, send, recv, c, c).wait_recv()

    stat[dp] = jnp.broadcast_to(jnp.sum(pooled, axis=1, keepdims=True), (sents, LANES))
    share(stat, s_send, s_recv)
    total = stat[0]
    for c in range(1, dps):
        total = total + stat[c]
    centered = pooled - total[:, 0:1] * (1.0 / d_model)
    narrow = centered.astype(BF16)
    sq = jnp.sum(centered * centered, axis=1, keepdims=True)
    gram[dp, 0] = jnp.zeros((sents, LANES), F32)
    gram[dp, 0, :, 0:sents] = lax.dot_general(narrow, narrow, CONTRACT_LAST, preferred_element_type=F32)
    gram[dp, 1] = jnp.broadcast_to(sq, (sents, LANES))
    share(gram, g_send, g_recv)
    products = gram[0, 0]
    sq = gram[0, 1]
    for c in range(1, dps):
        products = products + gram[c, 0]
        sq = sq + gram[c, 1]
    scale = lax.rsqrt(sq * (1.0 / d_model) + UNIT_FLOOR)
    r_i = lax.broadcasted_iota(jnp.int32, (sents, LANES), 0)
    c_i = lax.broadcasted_iota(jnp.int32, (sents, LANES), 1)
    across = jnp.sum(jnp.where(r_i == c_i, scale, 0.0), axis=0, keepdims=True)
    whole = 1.0 - products * scale * across * (1.0 / d_model)
    for r in range(each):
        row = jnp.sum(jnp.where(r_i == dp * each + r, whole, 0.0), axis=0, keepdims=True)
        out_ref[0, r:r + 1, :] = row[:, 0:sents]

    @pl.when(section == 0)
    def _():
        for h in range(SPLIT):
            for j in range(nj):
                for k in range(tensors):
                    if k:
                        spread(h, j, k).wait_send()
                    else:
                        @pl.when(tensor * nj + j != dp)
                        def _():
                            spread(h, j, k).wait_send()

    def drain(m, carry):
        for c in peers:
            rs_copy(m, c).wait_send()
            h_copy(m, dp, c).wait_send()
        for k in range(1, tensors):
            t_copy(m, tensor, lax.rem(tensor + k, tensors)).wait_send()

        @pl.when(section < sections - 1)
        def _():
            x_copy(m, section + 1).wait_send()
        return carry

    lax.fori_loop(0, micros, drain, 0)
    for c in peers:
        s_copy(lbuf, l_send, l_recv, dp, c).wait_send()
        s_copy(stat, s_send, s_recv, dp, c).wait_send()
        s_copy(gram, g_send, g_recv, dp, c).wait_send()


def per_device(hidden_in, norm_gain, gate_weight, up_weight, down_weight, lengths):
    sections = lax.axis_size("section")
    tensors = lax.axis_size("tensor")
    dps = lax.axis_size("dp")
    _, width, cols = gate_weight.shape
    micros = dps * SPLIT
    rows = hidden_in.shape[0] // SPLIT
    fc = cols // dps
    nj = hidden_in.shape[1] // width
    each = lengths.shape[0]
    sents = each * dps
    vm = pl.BlockSpec(memory_space=pltpu.VMEM)
    hbm = pl.BlockSpec(memory_space=pl.ANY)
    dma = pltpu.SemaphoreType.DMA
    smem = pl.BlockSpec(memory_space=pltpu.SMEM)
    return pl.pallas_call(
        functools.partial(kernel, dps, tensors, sections),
        out_shape=jax.ShapeDtypeStruct((1, each, sents), F32),
        in_specs=[vm] * 2 + [smem] + [hbm] * 3,
        out_specs=vm,
        scratch_shapes=[
            pltpu.VMEM((width, cols), BF16),
            pltpu.VMEM((width, cols), BF16),
            pltpu.VMEM((width, cols), BF16),
            pltpu.VMEM((micros, rows, width), BF16),
            pltpu.VMEM((micros, dps, rows, 2 * fc + LANES), BF16),
            pltpu.VMEM((micros, dps, rows, 2 * fc + LANES), BF16),
            pltpu.VMEM((micros, rows, 2 * fc), F32),
            pltpu.VMEM((micros, rows, LANES), F32),
            pltpu.VMEM((micros, dps, rows, fc), BF16),
            pltpu.VMEM((micros, tensors, rows, width), BF16),
            pltpu.VMEM((micros, rows, width), BF16),
            pltpu.VMEM((dps, sents, LANES), F32),
            pltpu.VMEM((dps, 2, sents, LANES), F32),
            pltpu.VMEM((dps, -(-each // 8) * 8, LANES), F32),
            pltpu.VMEM((sents, LANES), F32),
            dma((3, dps)),
            dma((SPLIT, nj * tensors)),
            dma((micros,)),
            dma((micros,)),
            dma((micros, dps)),
            dma((micros, dps)),
            dma((micros, dps)),
            dma((micros, dps)),
            dma((micros, tensors)),
            dma((micros, tensors)),
            dma((dps,)),
            dma((dps,)),
            dma((dps,)),
            dma((dps,)),
            dma((dps,)),
            dma((dps,)),
        ],
        compiler_params=pltpu.CompilerParams(
            collective_id=0, has_side_effects=True, vmem_limit_bytes=60 * 1024 * 1024),
    )(hidden_in, norm_gain, lengths, gate_weight, up_weight, down_weight)


def solution(mesh):
    placed = (
        P("dp", "tensor"),
        P("section", None),
        P("section", "dp", "tensor"),
        P("section", "dp", "tensor"),
        P("section", "dp", "tensor"),
        P("dp"),
    )
    return jax.shard_map(
        per_device, mesh=mesh, in_specs=placed, out_specs=P("section", "dp", None), check_vma=False
    )
```

```python
import functools

import jax
import jax.numpy as jnp
from jax import lax
from jax.experimental import pallas as pl
from jax.experimental.pallas import tpu as pltpu
from jax.sharding import PartitionSpec as P

RMS_EPS = 1e-05
UNIT_FLOOR = 0.1
CONTRACT_LAST = (((1,), (1,)), ((), ()))
MESH = pl.DeviceIdType.MESH
LANES = 128
F32 = jnp.float32
BF16 = jnp.bfloat16


SPLIT = 2


def pieces(fc):
    return 2 if fc % (2 * LANES) == 0 else 1


def kernel(dps, tensors, sections, hidden_ref, gain_ref, lens_ref, gate_hbm, up_hbm, down_hbm,
           out_ref, gate_v, up_v, down_v, x_in, rs_out, rs_in, own_gu, own_ss, hid, tx, outs, gram, lbuf, lens_full,
           w_sem, d_send, x_send, x_recv, rs_send, rs_recv, h_send, h_recv, t_send, t_recv,
           g_send, g_recv, l_send, l_recv):
    section = lax.axis_index("section")
    tensor = lax.axis_index("tensor")
    dp = lax.axis_index("dp")
    micros = dps * SPLIT
    width = gate_v.shape[0]
    cols = gate_v.shape[1]
    fc = cols // dps
    halves = pieces(fc)
    fh = fc // halves
    rows = x_in.shape[1]
    d_model = width * dps
    nj = hidden_ref.shape[1] // width

    def chunk(c):
        return pl.ds(pl.multiple_of(c * fc, fc), fc)

    def wcopy(which, c):
        src, dst = ((gate_hbm, gate_v), (up_hbm, up_v), (down_hbm, down_v))[which]
        return pltpu.make_async_copy(src.at[0, :, chunk(c)], dst.at[:, chunk(c)], w_sem.at[which, c])

    if dps == 4:
        mirror = dps - 1 - dp
        peers = [mirror, lax.rem(dp + 2, dps), lax.rem(mirror + 2, dps)]
    else:
        peers = [lax.rem(dp + k, dps) for k in range(1, dps)]
    order = peers + [dp]
    for c in order:
        wcopy(0, c).start()
        wcopy(1, c).start()
    for c in order:
        wcopy(2, c).start()

    barrier = pltpu.get_barrier_semaphore()
    for kt in range(tensors):
        for kd in range(dps):
            if kt or kd:
                pl.semaphore_signal(
                    barrier, inc=1,
                    device_id={"tensor": lax.rem(tensor + kt, tensors), "dp": lax.rem(dp + kd, dps)},
                    device_id_type=MESH)

    @pl.when(section > 0)
    def _():
        pl.semaphore_signal(barrier, inc=1, device_id={"section": section - 1}, device_id_type=MESH)

    @pl.when(section < sections - 1)
    def _():
        pl.semaphore_signal(barrier, inc=1, device_id={"section": section + 1}, device_id_type=MESH)

    pl.semaphore_wait(
        barrier,
        tensors * dps + 1 - jnp.where(section == 0, 1, 0) - jnp.where(section == sections - 1, 1, 0))

    each = lens_ref.shape[0]
    sents = each * dps
    slot = lax.broadcasted_iota(jnp.int32, lbuf.shape[1:], 0)
    own_lens = jnp.ones(lbuf.shape[1:], F32)
    for n in range(each):
        own_lens = jnp.where(slot == n, lens_ref[n].astype(F32), own_lens)
    lbuf[dp] = own_lens

    def s_copy(buf, send, recv, c, peer):
        return pltpu.make_async_remote_copy(
            src_ref=buf.at[c], dst_ref=buf.at[c], send_sem=send.at[peer], recv_sem=recv.at[c],
            device_id={"dp": peer}, device_id_type=MESH)

    def spread(h, j, k):
        return pltpu.make_async_remote_copy(
            src_ref=hidden_ref.at[pl.ds(h * rows, rows), pl.ds(j * width, width)],
            dst_ref=x_in.at[dp * SPLIT + h],
            send_sem=d_send.at[h, j * tensors + k], recv_sem=x_recv.at[dp * SPLIT + h],
            device_id={"tensor": lax.rem(tensor + k, tensors), "dp": tensor * nj + j}, device_id_type=MESH)

    @pl.when(section == 0)
    def _():
        for h in range(SPLIT):
            for j in range(nj):
                for k in range(tensors):
                    if k:
                        spread(h, j, k).start()
                    else:
                        @pl.when(tensor * nj + j != dp)
                        def _():
                            spread(h, j, k).start()

                        @pl.when(tensor * nj + j == dp)
                        def _():
                            x_in[dp * SPLIT + h] = hidden_ref[h * rows:(h + 1) * rows, j * width:(j + 1) * width]

    for c in peers:
        s_copy(lbuf, l_send, l_recv, dp, c).start()

    def base(q):
        return LANES + 2 * fh * q

    def piece(q):
        return pl.ds(0, base(1)) if q == 0 else pl.ds(base(q), 2 * fh)

    def rs_copy(m, c, q):
        return pltpu.make_async_remote_copy(
            src_ref=rs_out.at[m, c, :, piece(q)], dst_ref=rs_in.at[m, dp, :, piece(q)],
            send_sem=rs_send.at[m, c * halves + q], recv_sem=rs_recv.at[m, dp * halves + q],
            device_id={"dp": c}, device_id_type=MESH)

    def rs_wait(m, c, q):
        return pltpu.make_async_remote_copy(
            src_ref=rs_out.at[m, c, :, piece(q)], dst_ref=rs_in.at[m, c, :, piece(q)],
            send_sem=rs_send.at[m, c * halves + q], recv_sem=rs_recv.at[m, c * halves + q],
            device_id={"dp": c}, device_id_type=MESH)

    def h_copy(m, c, peer, q):
        part = hid.at[m, c, :, pl.ds(q * fh, fh)]
        return pltpu.make_async_remote_copy(
            src_ref=part, dst_ref=part,
            send_sem=h_send.at[m, peer * halves + q], recv_sem=h_recv.at[m, c * halves + q],
            device_id={"dp": peer}, device_id_type=MESH)

    def columns(c, q):
        return pl.ds(pl.multiple_of(c * fc + q * fh, fh), fh)

    def t_copy(m, c, peer):
        return pltpu.make_async_remote_copy(
            src_ref=tx.at[m, c], dst_ref=tx.at[m, c],
            send_sem=t_send.at[m, peer], recv_sem=t_recv.at[m, c],
            device_id={"tensor": peer}, device_id_type=MESH)

    def x_copy(m, to):
        return pltpu.make_async_remote_copy(
            src_ref=outs.at[m], dst_ref=x_in.at[m],
            send_sem=x_send.at[m], recv_sem=x_recv.at[m],
            device_id={"section": to}, device_id_type=MESH)

    lane = lax.broadcasted_iota(jnp.int32, (rows, LANES), 1)

    def gate_up(m):
        local = jnp.logical_and(section == 0, jnp.logical_and(m // SPLIT == dp, dp // nj == tensor))

        @pl.when(jnp.logical_not(local))
        def _():
            x_copy(m, section).wait_recv()

        x = x_in[m].astype(F32)
        ss = jnp.sum(x * x, axis=1, keepdims=True)
        high = ss.astype(BF16)
        low = (ss - high.astype(F32)).astype(BF16)
        packed = jnp.where(lane < LANES // 2, high.astype(F32), low.astype(F32)).astype(BF16)
        own_ss[m] = jnp.broadcast_to(ss, (rows, LANES))
        scaled = (x * gain_ref[:, pl.ds(pl.multiple_of(dp * width, width), width)]).astype(BF16)
        for c, q in [(c, q) for q in range(halves) for c in peers] + [(dp, q) for q in range(halves)]:
            if q == 0:
                @pl.when(m == 0)
                def _():
                    wcopy(0, c).wait()
                    wcopy(1, c).wait()

            g = jnp.dot(scaled, gate_v[:, columns(c, q)], preferred_element_type=F32)
            u = jnp.dot(scaled, up_v[:, columns(c, q)], preferred_element_type=F32)
            at = base(q)
            if c is not dp:
                if q == 0:
                    rs_out[m, c, :, 0:LANES] = packed
                rs_out[m, c, :, at:at + fh] = g.astype(BF16)
                rs_out[m, c, :, at + fh:at + 2 * fh] = u.astype(BF16)
                rs_copy(m, c, q).start()
            else:
                own_gu[m, :, q * 2 * fh:q * 2 * fh + fh] = g
                own_gu[m, :, q * 2 * fh + fh:(q + 1) * 2 * fh] = u

    def activate(m):
        inv = None
        for q in range(halves):
            for c in peers:
                rs_wait(m, c, q).wait_recv()
            if q == 0:
                ss = own_ss[m][:, 0:1]
                for c in peers:
                    ss = ss + jnp.sum(rs_in[m, c, :, 0:LANES].astype(F32), axis=1, keepdims=True) * (2.0 / LANES)
                inv = lax.rsqrt(ss * (1.0 / d_model) + RMS_EPS)
            g = own_gu[m, :, q * 2 * fh:q * 2 * fh + fh]
            u = own_gu[m, :, q * 2 * fh + fh:(q + 1) * 2 * fh]
            at = base(q)
            for c in peers:
                g = g + rs_in[m, c, :, at:at + fh].astype(F32)
                u = u + rs_in[m, c, :, at + fh:at + 2 * fh].astype(F32)
            g = g * inv
            u = u * inv
            hid[m, dp, :, q * fh:(q + 1) * fh] = (g / (1.0 + jnp.exp(-g)) * u).astype(BF16)
            for c in peers:
                h_copy(m, dp, c, q).start()

    def finish(m):
        acc = jnp.zeros((rows, width), F32)
        arrivals = [(dp, q) for q in range(halves)]
        arrivals += [(c, q) for q in range(halves) for c in peers[::2] + peers[1::2]]
        for c, q in arrivals:
            if c is not dp:
                h_copy(m, c, c, q).wait_recv()
            if q == 0:
                @pl.when(m == 0)
                def _():
                    wcopy(2, c).wait()

            acc = acc + lax.dot_general(hid[m, c, :, q * fh:(q + 1) * fh], down_v[:, columns(c, q)],
                                        CONTRACT_LAST, preferred_element_type=F32)
        tx[m, tensor] = acc.astype(BF16)
        for k in range(1, tensors):
            t_copy(m, tensor, lax.rem(tensor + k, tensors)).start()
        for k in range(1, tensors):
            other = lax.rem(tensor + k, tensors)
            t_copy(m, other, other).wait_recv()
        total = tx[m, 0].astype(F32)
        for t in range(1, tensors):
            total = total + tx[m, t].astype(F32)
        outs[m] = (x_in[m].astype(F32) + total).astype(BF16)

        @pl.when(section < sections - 1)
        def _():
            x_copy(m, section + 1).start()

    def step(i, carry):
        @pl.when(i < micros)
        def _():
            gate_up(i)

        @pl.when(i > 0)
        def _():
            finish(i - 1)

        @pl.when(i < micros)
        def _():
            activate(i)
        return carry

    lax.fori_loop(0, micros + 1, step, 0)

    for c in peers:
        s_copy(lbuf, l_send, l_recv, c, c).wait_recv()
    for c in range(dps):
        lens_full[c * each:(c + 1) * each] = lbuf[c, 0:each]
    tokens = micros * rows
    per = tokens // sents
    place = lax.broadcasted_iota(jnp.int32, (sents, tokens), 1) - per * lax.broadcasted_iota(
        jnp.int32, (sents, tokens), 0)
    lens = lens_full[:, 0:1]
    valid = jnp.logical_and(place >= 0, place.astype(F32) < lens)
    mask = jnp.where(valid, 1.0, 0.0).astype(BF16)
    pooled = jnp.dot(mask, outs[...].reshape(tokens, width), preferred_element_type=F32) / lens

    def share(buf, send, recv):
        for c in peers:
            s_copy(buf, send, recv, dp, c).start()
        for c in peers:
            s_copy(buf, send, recv, c, c).wait_recv()

    mean = jnp.sum(pooled, axis=1, keepdims=True) * (1.0 / width)
    centered = pooled - mean
    narrow = centered.astype(BF16)
    sq = jnp.sum(centered * centered, axis=1, keepdims=True)
    gram[dp, 0] = jnp.zeros((sents, LANES), F32)
    gram[dp, 0, :, 0:sents] = lax.dot_general(narrow, narrow, CONTRACT_LAST, preferred_element_type=F32)
    gram[dp, 1] = jnp.broadcast_to(sq, (sents, LANES))
    gram[dp, 2] = jnp.broadcast_to(mean, (sents, LANES))
    share(gram, g_send, g_recv)
    products, sq, mean = gram[0, 0], gram[0, 1], gram[0, 2]
    for c in range(1, dps):
        products = products + gram[c, 0]
        sq = sq + gram[c, 1]
        mean = mean + gram[c, 2]
    mean = mean * (1.0 / dps)
    r_i = lax.broadcasted_iota(jnp.int32, (sents, LANES), 0)
    c_i = lax.broadcasted_iota(jnp.int32, (sents, LANES), 1)
    for c in range(dps):
        off = gram[c, 2] - mean
        off_row = jnp.sum(jnp.where(r_i == c_i, off, 0.0), axis=0, keepdims=True)
        products = products + off * off_row * float(width)
        sq = sq + off * off * float(width)
    scale = lax.rsqrt(sq * (1.0 / d_model) + UNIT_FLOOR)
    across = jnp.sum(jnp.where(r_i == c_i, scale, 0.0), axis=0, keepdims=True)
    whole = 1.0 - products * scale * across * (1.0 / d_model)
    for r in range(each):
        row = jnp.sum(jnp.where(r_i == dp * each + r, whole, 0.0), axis=0, keepdims=True)
        out_ref[0, r:r + 1, :] = row[:, 0:sents]

    @pl.when(section == 0)
    def _():
        for h in range(SPLIT):
            for j in range(nj):
                for k in range(tensors):
                    if k:
                        spread(h, j, k).wait_send()
                    else:
                        @pl.when(tensor * nj + j != dp)
                        def _():
                            spread(h, j, k).wait_send()

    def drain(m, carry):
        for c in peers:
            for q in range(halves):
                rs_copy(m, c, q).wait_send()
                h_copy(m, dp, c, q).wait_send()
        for k in range(1, tensors):
            t_copy(m, tensor, lax.rem(tensor + k, tensors)).wait_send()

        @pl.when(section < sections - 1)
        def _():
            x_copy(m, section + 1).wait_send()
        return carry

    lax.fori_loop(0, micros, drain, 0)
    for c in peers:
        s_copy(lbuf, l_send, l_recv, dp, c).wait_send()
        s_copy(gram, g_send, g_recv, dp, c).wait_send()


def per_device(hidden_in, norm_gain, gate_weight, up_weight, down_weight, lengths):
    sections = lax.axis_size("section")
    tensors = lax.axis_size("tensor")
    dps = lax.axis_size("dp")
    _, width, cols = gate_weight.shape
    micros = dps * SPLIT
    rows = hidden_in.shape[0] // SPLIT
    fc = cols // dps
    halves = pieces(fc)
    nj = hidden_in.shape[1] // width
    each = lengths.shape[0]
    sents = each * dps
    vm = pl.BlockSpec(memory_space=pltpu.VMEM)
    hbm = pl.BlockSpec(memory_space=pl.ANY)
    dma = pltpu.SemaphoreType.DMA
    smem = pl.BlockSpec(memory_space=pltpu.SMEM)
    return pl.pallas_call(
        functools.partial(kernel, dps, tensors, sections),
        out_shape=jax.ShapeDtypeStruct((1, each, sents), F32),
        in_specs=[vm] * 2 + [smem] + [hbm] * 3,
        out_specs=vm,
        scratch_shapes=[
            pltpu.VMEM((width, cols), BF16),
            pltpu.VMEM((width, cols), BF16),
            pltpu.VMEM((width, cols), BF16),
            pltpu.VMEM((micros, rows, width), BF16),
            pltpu.VMEM((micros, dps, rows, 2 * fc + LANES), BF16),
            pltpu.VMEM((micros, dps, rows, 2 * fc + LANES), BF16),
            pltpu.VMEM((micros, rows, 2 * fc), F32),
            pltpu.VMEM((micros, rows, LANES), F32),
            pltpu.VMEM((micros, dps, rows, fc), BF16),
            pltpu.VMEM((micros, tensors, rows, width), BF16),
            pltpu.VMEM((micros, rows, width), BF16),
            pltpu.VMEM((dps, 3, sents, LANES), F32),
            pltpu.VMEM((dps, -(-each // 8) * 8, LANES), F32),
            pltpu.VMEM((sents, LANES), F32),
            dma((3, dps)),
            dma((SPLIT, nj * tensors)),
            dma((micros,)),
            dma((micros,)),
            dma((micros, dps * halves)),
            dma((micros, dps * halves)),
            dma((micros, dps * halves)),
            dma((micros, dps * halves)),
            dma((micros, tensors)),
            dma((micros, tensors)),
            dma((dps,)),
            dma((dps,)),
            dma((dps,)),
            dma((dps,)),
        ],
        compiler_params=pltpu.CompilerParams(
            collective_id=0, has_side_effects=True, vmem_limit_bytes=60 * 1024 * 1024),
    )(hidden_in, norm_gain, lengths, gate_weight, up_weight, down_weight)


def solution(mesh):
    placed = (
        P("dp", "tensor"),
        P("section", None),
        P("section", "dp", "tensor"),
        P("section", "dp", "tensor"),
        P("section", "dp", "tensor"),
        P("dp"),
    )
    return jax.shard_map(
        per_device, mesh=mesh, in_specs=placed, out_specs=P("section", "dp", None), check_vma=False
    )
```
